128 devices in a mesh: flow: 16 (over y, x_hi, core), cross: 8 (over x_lo, z).
Axes of the slice: x: 4 (x_hi: 2, x_lo: 2; x = x_hi * 2 + x_lo), y: 4, z: 4, core: 2. Of those that a mesh axis runs over, the one named last changes fastest.
Arguments:
- solid_temp: float32 [8, 4096, 4096], P(None, 'flow', 'cross'), may hold values from 0.5 to 1.5
- conductance: float32 [8, 4096, 4096], P(None, 'flow', 'cross'), may hold values from 0.03 to 0.12
- coolant: float32 [4, 4096, 4096], P(None, 'flow', 'cross'), may hold values from 0 to 1
- power_index: int32 [4096, 4096], P('flow', 'cross'), may hold values from 0 to 15
- power_levels: float32 [16], replicated, may hold values from 0.05 to 0.5
- channel_mask: int32 [4, 4096], P(None, 'cross'), may hold values 0 or 1
- inlet: float32 [4, 4096], P(None, 'cross'), may hold values from 0 to 0.5
- flow_gain: float32 [4, 4096], P(None, 'cross'), may hold values from 2 to 16
Outputs:
- solid_next: float32 [8, 4096, 4096], P(None, 'flow', 'cross')
- coolant_next: float32 [4, 4096, 4096], P(None, 'flow', 'cross')
The draws below stay inside these ranges and needn't reach their ends.
All inputs are finite; a program needn't handle non-finite values. No bound on the sum of `channel_mask` on one device may be relied on, other than what follows from the above.
Results may differ from the reference program's by a relative error of at most 0.000058.
Values sent between devices are 32-bit elements; how exact they have to be, the bound alone decides.
No kernel may reach another device: no remote copies, remote signals or barrier semaphores. Data moves between devices by JAX's collectives and lax.ppermute only.
A program may use at most 128 MiB of HBM per device.

```python
import math
import jax
import jax.numpy as jnp

SOLID = 8
CHAN = 4
LEVELS = 16
NX = 4096
NY = 4096


def plant(drawn, stream_key, low, largest):
    spot = [jax.random.randint(jax.random.fold_in(stream_key, axis), (), 0, length) for axis, length in enumerate(drawn.shape)]
    widest = drawn.shape.index(max(drawn.shape))
    beside = spot[:widest] + [(spot[widest] + 1) % drawn.shape[widest]] + spot[widest + 1:]
    return drawn.at[tuple(spot)].set(low).at[tuple(beside)].set(largest)


def steps_of(rng, dims, split, least, top_value):
    def one(position, shards_of):
        heights = jax.random.uniform(jax.random.fold_in(jax.random.fold_in(rng, 6), position), (shards_of,), jnp.float32, least / len(split), top_value / len(split))
        return jnp.repeat(jnp.exp(heights), dims[position] // shards_of).reshape((-1,) + (1,) * (len(dims) - position - 1))

    gain = one(*split[0])
    for cut in split[1:]:
        gain = gain * one(*cut)
    return gain


def setup_inputs(seed: int = 0) -> dict:
    arg_keys = jax.random.split(jax.random.key(seed), 9)
    solid_temp = jnp.clip(0.5 + 1.0 * jax.random.uniform(arg_keys[0], (SOLID, NX, NY), jnp.float32) ** steps_of(arg_keys[0], (SOLID, NX, NY), ((1, 16), (2, 8)), -0.2, 0.2), 0.5, 1.5)
    conductance = jnp.clip(jnp.exp(math.log(0.12) - 1.3862944 * jax.random.uniform(arg_keys[1], (SOLID, NX, NY), jnp.float32) ** steps_of(arg_keys[1], (SOLID, NX, NY), ((1, 16), (2, 8)), -0.2, 0.2)), 0.03, 0.12)
    coolant = jnp.clip(1.0 * jax.random.uniform(arg_keys[2], (CHAN, NX, NY), jnp.float32) ** steps_of(arg_keys[2], (CHAN, NX, NY), ((1, 16), (2, 8)), -0.2, 0.2), 0.0, 1.0)
    power_index = plant(jax.random.randint(arg_keys[3], (NX, NY), 0, LEVELS), jax.random.fold_in(arg_keys[3], 1), 0, LEVELS - 1).astype(jnp.int32)
    power_levels = jnp.clip(jnp.exp(jax.random.uniform(arg_keys[4], (LEVELS,), jnp.float32, math.log(0.05), math.log(0.5))), 0.05, 0.5)
    channel_mask = plant((jax.random.randint(arg_keys[5], (CHAN, NY), 0, 2) < 1).astype(jnp.int32), jax.random.fold_in(arg_keys[5], 1), 0, 1)
    inlet = jnp.clip(0.5 * jax.random.uniform(arg_keys[6], (CHAN, NY), jnp.float32) ** steps_of(arg_keys[6], (CHAN, NY), ((1, 8),), -0.2, 0.2), 0.0, 0.5)
    flow_gain = jnp.clip(jnp.exp(math.log(16.0) - 2.0794415 * jax.random.uniform(arg_keys[7], (CHAN, NY), jnp.float32) ** steps_of(arg_keys[7], (CHAN, NY), ((1, 8),), -0.2, 0.2)), 2.0, 16.0)
    return dict(solid_temp=solid_temp, conductance=conductance, coolant=coolant, power_index=power_index, power_levels=power_levels, channel_mask=channel_mask, inlet=inlet, flow_gain=flow_gain)


def advance(padded, conduct, heating, coolant_now, open_cols):
    center = padded[:, 1:-1, 1:-1]
    lateral = padded[:, 2:, 1:-1] + padded[:, :-2, 1:-1] + padded[:, 1:-1, 2:] + padded[:, 1:-1, :-2]
    upward = center[1:] - center[:-1]
    no_layer = jnp.zeros_like(center[:1])
    vertical = jnp.concatenate([upward, no_layer], axis=0) - jnp.concatenate([no_layer, upward], axis=0)
    chans = coolant_now.shape[0]
    paired = center.reshape(chans, 2, center.shape[1], center.shape[2])
    film_term = 0.08 * open_cols[:, None, None, :] * (coolant_now[:, None] - paired)
    source = jnp.concatenate([heating[None], jnp.zeros_like(center[1:])], axis=0)
    return center + conduct * (lateral - 4.0 * center) + 0.05 * vertical + film_term.reshape(center.shape) + source


def reference(solid_temp, conductance, coolant, power_index, power_levels, channel_mask, inlet, flow_gain):
    heating = power_levels[power_index]
    open_cols = channel_mask.astype(jnp.float32)
    current = solid_temp
    for repeat in range(2):
        padded = jnp.pad(current, ((0, 0), (1, 1), (1, 1)))
        current = advance(padded, conductance, heating, coolant, open_cols)
    paired = current.reshape(coolant.shape[0], 2, current.shape[1], current.shape[2])
    absorbed = 0.08 * open_cols[:, None, :] * (paired[:, 0] + paired[:, 1] - 2.0 * coolant)
    upstream = jnp.cumsum(absorbed, axis=1) - 0.5 * absorbed
    fluid_new = inlet[:, None, :] + flow_gain[:, None, :] * upstream / NX
    return current, fluid_new
```

```python
import functools

import jax
import jax.numpy as jnp
from jax import lax
from jax.experimental import pallas as pl
from jax.experimental.pallas import tpu as pltpu
from jax.sharding import PartitionSpec as P

LANES = 128
SUB = 8
VERTICAL = 0.05
FILM = 0.08
VMEM = pl.BlockSpec(memory_space=pltpu.VMEM)
SMEM = pl.BlockSpec(memory_space=pltpu.SMEM)
HBM = pl.BlockSpec(memory_space=pltpu.HBM)


def cut(c):
    return slice(c * LANES, (c + 1) * LANES)


def iota(dim):
    return lax.broadcasted_iota(jnp.int32, (SUB, LANES), dim)


def looked_up(index, levels_ref):
    values = [levels_ref[i] for i in range(levels_ref.shape[0])]
    bit = 0
    while len(values) > 1:
        odd = (index & (1 << bit)) != 0
        values = [jnp.where(odd, b, a) for a, b in zip(values[::2], values[1::2])]
        bit += 1
    return values[0]


def parity(axis):
    return lax.rem(lax.axis_index(axis), 2)


def edge_rows(levels_ref, s_ref, c_ref, w_ref, p_ref, even_ref, odd_ref, s_buf, c_buf, w_buf, p_buf, sems):
    layers, length, _ = s_ref.shape
    chans = w_ref.shape[0]
    copies = []
    for side, at in ((0, 0), (1, length - SUB)):
        for n, (src, dst) in enumerate(((s_ref, s_buf), (c_ref, c_buf), (w_ref, w_buf), (p_ref, p_buf))):
            view = src.at[pl.ds(at, SUB), :] if n == 3 else src.at[:, pl.ds(at, SUB), :]
            copies.append(pltpu.make_async_copy(view, dst.at[side], sems.at[side, n]))
            copies[-1].start()
    for copy in copies:
        copy.wait()

    def fill(out, side, near, far):
        for l in range(layers):
            out[l : l + 1, :] = s_buf[side, l, near : near + 1, :]
            out[layers + l : layers + l + 1, :] = s_buf[side, l, far : far + 1, :]
            out[2 * layers + l : 2 * layers + l + 1, :] = c_buf[side, l, near : near + 1, :]
        for k in range(chans):
            out[3 * layers + k : 3 * layers + k + 1, :] = w_buf[side, k, near : near + 1, :]
        heat = looked_up(p_buf[side, near : near + 1, :], levels_ref)
        for k in range(chans):
            out[3 * layers + chans + k : 3 * layers + chans + k + 1, :] = heat

    par = parity("flow")

    @pl.when(par == 0)
    def _():
        fill(even_ref, 1, 7, 6)
        fill(odd_ref, 0, 0, 1)

    @pl.when(par != 0)
    def _():
        fill(odd_ref, 1, 7, 6)
        fill(even_ref, 0, 0, 1)


def set_film(mask_ref, film):
    for k in range(mask_ref.shape[0]):
        row = mask_ref[k : k + 1, :].astype(jnp.float32) * FILM
        film[k] = jnp.broadcast_to(row, film.shape[1:])


def stencil(l, load, c_ref, w_ref, film, top, bottom, sides, emit, length, layers, tiles):
    row, lane = iota(0), iota(1)
    k = l // 2
    above_l, below_l = jnp.maximum(l - 1, 0), jnp.minimum(l + 1, layers - 1)
    f = [film[k, :, cut(c)] for c in range(tiles)]
    keep = [(1.0 - 2.0 * VERTICAL) - v for v in f]
    count = length // SUB
    down = lambda v: pltpu.roll(v, 1, 0)
    up = lambda v: pltpu.roll(v, SUB - 1, 0)
    if top is None:
        before = [jnp.zeros((SUB, LANES), jnp.float32)] * tiles
        final = before
    else:
        before = [top[l, :, cut(c)] for c in range(tiles)]
        final = None
    u = [load(l, 0, c) for c in range(tiles)]
    u_up = [up(v) for v in u]
    for r in range(count):
        if r + 1 < count:
            after = [load(l, (r + 1) * SUB, c) for c in range(tiles)]
            after_up = [up(v) for v in after]
        elif final is None:
            after = [bottom[l, :, cut(c)] for c in range(tiles)]
            after_up = after
        else:
            after = after_up = final
        u_down = [down(v) for v in u]
        east = [pltpu.roll(v, 1, 1) for v in u]
        west = [pltpu.roll(v, LANES - 1, 1) for v in u]
        left, right = sides(r)
        at = r * SUB
        conds, outs, ws = [], [], []
        for c in range(tiles):
            n = jnp.where(row == 0, before[c], u_down[c])
            s = jnp.where(row == SUB - 1, after_up[c], u_up[c])
            lf = jnp.where(lane == 0, left if c == 0 else east[c - 1], east[c])
            rt = jnp.where(lane == LANES - 1, right if c == tiles - 1 else west[c + 1], west[c])
            cond = c_ref[l, at : at + SUB, cut(c)]
            w = w_ref[k, at : at + SUB, cut(c)]
            around = ((n + s) + (lf + rt)) - 4.0 * u[c]
            beside = load(above_l, at, c) + load(below_l, at, c)
            outs.append((keep[c] * u[c] + cond * around) + (VERTICAL * beside + f[c] * w))
            conds.append(cond)
            ws.append(w)
        emit(r, u, conds, outs, ws)
        before, u, u_up = u_down, after, after_up


def first_step(levels_ref, s_ref, c_ref, w_ref, p_ref, mask_ref, s1_ref, heat_ref, flat_ref, film):
    layers, length, width = s_ref.shape
    tiles = width // LANES
    zero = jnp.zeros((SUB, LANES), jnp.float32)
    set_film(mask_ref, film)

    def layer(l, carry):
        def load(m, at, c):
            return s_ref[m, at : at + SUB, cut(c)]

        def emit(r, u, conds, outs, ws):
            at = r * SUB
            for c in range(tiles):
                s1_ref[l, at : at + SUB, cut(c)] = outs[c]

        stencil(l, load, c_ref, w_ref, film, None, None, lambda r: (zero, zero), emit, length, layers, tiles)
        return carry

    lax.fori_loop(0, layers, layer, 0)
    for r in range(length // SUB):
        at = r * SUB
        for c in range(tiles):
            heat = looked_up(p_ref[at : at + SUB, cut(c)], levels_ref)
            heat_ref[at : at + SUB, cut(c)] = heat
            s1_ref[0, at : at + SUB, cut(c)] += heat
    for n, ref in enumerate((s_ref, c_ref, s1_ref)):
        for l in range(layers):
            for side in range(2):
                turned = ref[l, :, cut(side * (tiles - 1))].T
                j = 64 * side + n * SUB + l
                flat_ref[j : j + 1, :] = turned[0:1, :] if side == 0 else turned[LANES - 1 :, :]


def add_rows(s_ref, c_ref, mask_ref, re_ref, ro_ref, flat_ref, s1_in, s1_ref, halo_ref, even_ref, odd_ref, rows):
    layers, length, width = s_ref.shape
    chans = mask_ref.shape[0]
    tiles = width // LANES
    last = tiles - 1
    row, lane = iota(0), iota(1)
    zero = jnp.zeros((SUB, LANES), jnp.float32)
    fpar, cpar = parity("flow"), parity("cross")
    for l in range(layers):
        rows[0, l : l + 1, :] = s_ref[l, 0:1, :]
        rows[1, l : l + 1, :] = s_ref[l, length - 1 : length, :]
        rows[2, l : l + 1, :] = mask_ref[l // 2 : l // 2 + 1, :].astype(jnp.float32) * FILM

    top = lambda a, b, c: jnp.where(fpar == 0, ro_ref[a:b, cut(c)], re_ref[a:b, cut(c)])
    bottom = lambda a, b, c: jnp.where(fpar == 0, re_ref[a:b, cut(c)], ro_ref[a:b, cut(c)])
    nears = []
    for side, halo in ((0, top), (1, bottom)):
        near = [halo(0, layers, c) for c in range(tiles)]
        nears.append(near)
        east = [pltpu.roll(v, 1, 1) for v in near]
        west = [pltpu.roll(v, LANES - 1, 1) for v in near]
        at = 0 if side == 0 else length - SUB
        for c in range(tiles):
            cond = halo(2 * layers, 3 * layers, c)
            rest = halo(3 * layers, 4 * layers, c)
            heat = jnp.where(row == 0, jnp.broadcast_to(rest[chans : chans + 1, :], (SUB, LANES)), 0.0)
            cool = zero
            for k in range(chans):
                cool = jnp.where(row // 2 == k, jnp.broadcast_to(rest[k : k + 1, :], (SUB, LANES)), cool)
            u = near[c]
            lf = jnp.where(lane == 0, zero if c == 0 else east[c - 1], east[c])
            rt = jnp.where(lane == LANES - 1, zero if c == last else west[c + 1], west[c])
            around = (halo(layers, 2 * layers, c) + rows[side, :, cut(c)]) + (lf + rt)
            over = jnp.where(row == 0, u, pltpu.roll(u, 1, 0))
            under = jnp.where(row == SUB - 1, u, pltpu.roll(u, SUB - 1, 0))
            halo_ref[side * layers : (side + 1) * layers, cut(c)] = (
                u
                + cond * (around - 4.0 * u)
                + VERTICAL * ((over - u) + (under - u))
                + rows[2, :, cut(c)] * (cool - u)
                + heat
            )
            spot = 0 if side == 0 else SUB - 1
            for l in range(layers):
                outside = jnp.broadcast_to(u[l : l + 1, :], (SUB, LANES))
                more = jnp.where(row == spot, c_ref[l, at : at + SUB, cut(c)] * outside, 0.0)
                s1_ref[l, at : at + SUB, cut(c)] = s1_in[l, at : at + SUB, cut(c)] + more

    back = LANES - 1
    def fill(right_ref, left_ref):
        for is_left, out in ((0, right_ref), (1, left_ref)):
            base = 0 if is_left else 64
            tile = 0 if is_left else last
            out[0:16, :] = flat_ref[base : base + 16, :]
            t, b = nears[0][tile], nears[1][tile]
            t0 = t if is_left else pltpu.roll(t, 1, 1)
            b1 = pltpu.roll(b, back, 1) if is_left else b
            out[16:24, 0:LANES] = flat_ref[base + 16 : base + 24, 0:LANES] + jnp.where(
                lane == 0, flat_ref[base + 8 : base + 16, 0:LANES] * t0, 0.0
            )
            out[16:24, LANES:] = flat_ref[base + 16 : base + 24, LANES:] + jnp.where(
                lane == back, flat_ref[base + 8 : base + 16, LANES:] * b1, 0.0
            )
            shift = back if is_left else 1
            out[24:32, 0:LANES] = pltpu.roll(t, shift, 1)
            out[24:32, LANES:] = pltpu.roll(b, shift, 1)

    @pl.when(cpar == 0)
    def _():
        fill(even_ref, odd_ref)

    @pl.when(cpar != 0)
    def _():
        fill(odd_ref, even_ref)


def second_step(
    s1_ref, c_ref, w_ref, heat_ref, mask_ref, re_ref, ro_ref, halo_ref, own_ref, ce_ref, co_ref,
    s2_ref, absorbed_out, total_ref, film, top, bottom, edge, columns, sums_ref, out_buf, absorbed_ref, sem, absorbed_sem,
):
    layers, length, width = s1_ref.shape
    chans = w_ref.shape[0]
    tiles = width // LANES
    last_tile = tiles - 1
    lane = iota(1)
    fpar, cpar = parity("flow"), parity("cross")
    set_film(mask_ref, film)
    got_left = jnp.where(cpar == 0, co_ref[...], ce_ref[...])
    got_right = jnp.where(cpar == 0, ce_ref[...], co_ref[...])
    row = iota(0)
    middle = jnp.zeros((LANES - 2 * SUB, LANES), jnp.float32)
    beyond = (
        (got_left[0:8, :], got_right[0:8, :]),
        (
            got_left[16:24, :] + got_left[8:16, :] * own_ref[0:8, :],
            got_right[16:24, :] + got_right[8:16, :] * own_ref[64:72, :],
        ),
    )
    for n, (lefts, rights) in enumerate(beyond):
        for l in range(layers):
            for half in range(length // LANES):
                first = jnp.where(row == 0, jnp.broadcast_to(lefts[l : l + 1, cut(half)], (SUB, LANES)), 0.0)
                final = jnp.where(row == SUB - 1, jnp.broadcast_to(rights[l : l + 1, cut(half)], (SUB, LANES)), 0.0)
                turned = jnp.concatenate([first, middle, final], axis=0).T
                columns[n, l, half * LANES : (half + 1) * LANES, :] = turned

    cond_top = jnp.where(fpar == 0, ro_ref[16:24, :], re_ref[16:24, :])
    cond_bottom = jnp.where(fpar == 0, re_ref[16:24, :], ro_ref[16:24, :])
    for at, out, cond in ((0, top, cond_top), (1, bottom, cond_bottom)):
        for c in range(tiles):
            value = halo_ref[at * layers : (at + 1) * layers, cut(c)]
            if c == 0:
                value += cond[:, cut(c)] * jnp.where(lane == 0, got_left[24:32, cut(at)], 0.0)
            if c == last_tile:
                value += cond[:, cut(c)] * jnp.where(lane == LANES - 1, got_right[24:32, cut(at)], 0.0)
            for l in range(layers):
                out[l, :, cut(c)] = jnp.broadcast_to(value[l : l + 1, :], (SUB, LANES))

    def complete(l, carry):
        for r in range(length // SUB):
            at = r * SUB
            beside = columns[0, l, at : at + SUB, :]
            for e, c, spot in ((0, 0, 0), (1, last_tile, LANES - 1)):
                more = c_ref[l, at : at + SUB, cut(c)] * jnp.where(lane == spot, beside, 0.0)
                edge[e, l, at : at + SUB, :] = s1_ref[l, at : at + SUB, cut(c)] + more
        return carry

    lax.fori_loop(0, layers, complete, 0)

    def load(m, at, c):
        if c == 0:
            return edge[0, m, at : at + SUB, :]
        if c == last_tile:
            return edge[1, m, at : at + SUB, :]
        return s1_ref[m, at : at + SUB, cut(c)]

    def layer(l, carry):
        def sides(r):
            beside = columns[1, l, r * SUB : (r + 1) * SUB, :]
            return beside, beside

        def emit(r, u, conds, outs, ws):
            at = r * SUB
            for c in range(tiles):
                out = outs[c]
                out_buf[l, at : at + SUB, cut(c)] = out

        stencil(l, load, c_ref, w_ref, film, top, bottom, sides, emit, length, layers, tiles)

        @pl.when(l == 0)
        def _():
            for r in range(length // SUB):
                at = r * SUB
                out_buf[0, at : at + SUB, :] += heat_ref[at : at + SUB, :]

        pltpu.make_async_copy(out_buf.at[l], s2_ref.at[l], sem.at[l]).start()

        @pl.when(lax.rem(l, 2) == 1)
        def _():
            k = l // 2
            for c in range(tiles):
                f = film[k, :, cut(c)]
                total = [jnp.zeros((SUB, LANES), jnp.float32)] * 4
                for r in range(length // SUB):
                    at = r * SUB
                    pair = out_buf[l - 1, at : at + SUB, cut(c)] + out_buf[l, at : at + SUB, cut(c)]
                    value = f * (pair - 2.0 * w_ref[k, at : at + SUB, cut(c)])
                    absorbed_ref[k, at : at + SUB, cut(c)] = value
                    total[r % 4] = total[r % 4] + value
                sums_ref[k, :, cut(c)] = (total[0] + total[1]) + (total[2] + total[3])
            pltpu.make_async_copy(absorbed_ref.at[k], absorbed_out.at[k], absorbed_sem.at[k]).start()

        return carry

    lax.fori_loop(0, layers, layer, 0)
    for k in range(chans):
        row_sum = jnp.sum(sums_ref[k], axis=0, keepdims=True)
        for j in range(total_ref.shape[0]):
            total_ref[j, 0, k : k + 1, :] = row_sum
    for l in range(layers):
        pltpu.make_async_copy(out_buf.at[l], s2_ref.at[l], sem.at[l]).wait()
    for k in range(chans):
        pltpu.make_async_copy(absorbed_ref.at[k], absorbed_out.at[k], absorbed_sem.at[k]).wait()


def march(length_cells, absorbed_ref, inlet_ref, gain_ref, part_ref):
    chans, length, _ = absorbed_ref.shape
    i = lax.broadcasted_iota(jnp.int32, (length, length), 0)
    j = lax.broadcasted_iota(jnp.int32, (length, length), 1)
    triangle = jnp.where(j < i, 1.0, jnp.where(j == i, 0.5, 0.0)).astype(jnp.bfloat16)
    for k in range(chans):
        absorbed = absorbed_ref[k]
        within = None
        for _ in range(3):
            term = absorbed.astype(jnp.bfloat16)
            absorbed = absorbed - term.astype(jnp.float32)
            product = jnp.dot(triangle, term, preferred_element_type=jnp.float32)
            within = product if within is None else within + product
        scale = gain_ref[k : k + 1, :] * (1.0 / length_cells)
        part_ref[k] = inlet_ref[k : k + 1, :] + scale * within


def finish(length_cells, part_ref, every_ref, gain_ref, out_ref, buf, sem):
    flow = lax.axis_index("flow")
    total = jnp.zeros(gain_ref.shape, jnp.float32)
    for j in range(every_ref.shape[0]):
        total += jnp.where(j < flow, every_ref[j, 0], 0.0)
    carried = total * gain_ref[...] * (1.0 / length_cells)
    chans = part_ref.shape[0]
    copies = []
    for k in range(chans):
        buf[k] = part_ref[k] + carried[k : k + 1, :]
        copies.append(pltpu.make_async_copy(buf.at[k], out_ref.at[k], sem.at[k]))
        copies[-1].start()
    for copy in copies:
        copy.wait()


def swaps(size):
    even = [(i, i ^ 1) for i in range(size)]
    odd = [(i, i + 1 if i % 2 else i - 1) for i in range(1, size - 1)]
    return even, odd


def f32(*dims):
    return jax.ShapeDtypeStruct(dims, jnp.float32)


def call(kernel, name, out_shape, in_specs, out_specs, scratch, mib, flops, **kw):
    return pl.pallas_call(
        kernel,
        out_shape=out_shape,
        in_specs=in_specs,
        out_specs=out_specs,
        scratch_shapes=scratch,
        compiler_params=pltpu.CompilerParams(vmem_limit_bytes=int(mib * 2**20)),
        cost_estimate=pl.CostEstimate(flops=int(flops), bytes_accessed=0, transcendentals=0),
        name=name,
        **kw,
    )


def shards(s0, cond, cool, index, levels, mask, inlet, gain):
    layers, length, width = s0.shape
    chans = cool.shape[0]
    flows = lax.axis_size("flow")
    count = 4 * layers
    block = f32(layers, length, width)
    buf = lambda *dims: pltpu.VMEM(dims, jnp.float32)
    hbm = lambda *dims: pltpu.HBM(dims, jnp.float32)
    dma = lambda *dims: pltpu.SemaphoreType.DMA(dims)
    in_hbm = lambda x: pltpu.with_memory_space_constraint(x, pltpu.HBM)
    even, odd = call(
        edge_rows, "edge_rows", (f32(count, width), f32(count, width)), [SMEM] + [HBM] * 4, (VMEM, VMEM),
        [
            buf(2, layers, SUB, width), buf(2, layers, SUB, width), buf(2, chans, SUB, width),
            pltpu.VMEM((2, SUB, width), jnp.int32), dma(2, 4),
        ],
        4, 1e5,
    )(levels, in_hbm(s0), in_hbm(cond), in_hbm(cool), in_hbm(index))
    even_pairs, odd_pairs = swaps(flows)
    row_odd = lax.ppermute(odd, "flow", odd_pairs)
    row_even = lax.ppermute(even, "flow", even_pairs)

    work = 20 * layers * length * width
    s1, heat, own = call(
        first_step, "first_step", (block, f32(length, width), f32(LANES, length)), [SMEM] + [VMEM] * 5, (VMEM,) * 3,
        [buf(chans, SUB, width)], 17, work,
    )(levels, s0, cond, cool, index, mask)
    s1, halo, even, odd = call(
        add_rows, "add_rows", (block, f32(2 * layers, width), f32(32, length), f32(32, length)), [VMEM] * 7, (VMEM,) * 4,
        [buf(3, layers, width)], 17, 1e5, input_output_aliases={6: 0},
    )(s0, cond, mask, row_even, row_odd, own, s1)
    even_pairs, odd_pairs = swaps(lax.axis_size("cross"))
    col_odd = lax.ppermute(odd, "cross", odd_pairs)
    col_even = lax.ppermute(even, "cross", even_pairs)

    s2, absorbed, totals = call(
        second_step, "second_step",
        (hbm(layers, length, width), hbm(chans, length, width), f32(flows, 1, chans, width)),
        [VMEM] * 11, (HBM, HBM, VMEM),
        [
            buf(chans, SUB, width), buf(layers, SUB, width), buf(layers, SUB, width), buf(2, layers, length, LANES),
            buf(2, layers, length, LANES), buf(chans, SUB, width), buf(layers, length, width), buf(chans, length, width), dma(layers), dma(chans),
        ],
        22, work,
    )(s1, cond, cool, heat, mask, row_even, row_odd, halo, own, col_even, col_odd)
    everyone = lax.all_to_all(totals, "flow", 0, 0, tiled=True)

    cells = float(length * flows)
    part = call(
        functools.partial(march, cells), "march", f32(chans, length, width), [VMEM] * 3, VMEM, [], 10, work // 4,
    )(absorbed, inlet, gain)
    fluid = call(
        functools.partial(finish, cells), "finish", hbm(chans, length, width), [VMEM] * 3, HBM,
        [buf(chans, length, width), dma(chans)], 6, 1e5,
    )(part, everyone, gain)
    return s2, fluid


def solution(mesh):
    return jax.shard_map(
        shards,
        mesh=mesh,
        in_specs=(
            P(None, "flow", "cross"),
            P(None, "flow", "cross"),
            P(None, "flow", "cross"),
            P("flow", "cross"),
            P(),
            P(None, "cross"),
            P(None, "cross"),
            P(None, "cross"),
        ),
        out_specs=(P(None, "flow", "cross"), P(None, "flow", "cross")),
        check_vma=False,
    )
```

```python
import functools

import jax
import jax.numpy as jnp
from jax import lax
from jax.experimental import pallas as pl
from jax.experimental.pallas import tpu as pltpu
from jax.sharding import PartitionSpec as P

LANES = 128
SUB = 8
VERTICAL = 0.05
FILM = 0.08
VMEM = pl.BlockSpec(memory_space=pltpu.VMEM)
SMEM = pl.BlockSpec(memory_space=pltpu.SMEM)
HBM = pl.BlockSpec(memory_space=pltpu.HBM)


def cut(c):
    return slice(c * LANES, (c + 1) * LANES)


def iota(dim):
    return lax.broadcasted_iota(jnp.int32, (SUB, LANES), dim)


def looked_up(index, levels_ref):
    values = [levels_ref[i] for i in range(levels_ref.shape[0])]
    bit = 0
    while len(values) > 1:
        odd = (index & (1 << bit)) != 0
        values = [jnp.where(odd, b, a) for a, b in zip(values[::2], values[1::2])]
        bit += 1
    return values[0]


def parity(axis):
    return lax.rem(lax.axis_index(axis), 2)


def edge_rows(
    levels_ref, s_ref, c_ref, w_ref, p_ref, mask_ref, even_ref, odd_ref, film_ref,
    s_buf, c_buf, w_buf, p_buf, mask_buf, levels_buf, sems, more_sems,
):
    layers, length, _ = s_ref.shape
    chans = w_ref.shape[0]
    copies = []
    for side, at in ((0, 0), (1, length - SUB)):
        for n, (src, dst) in enumerate(((s_ref, s_buf), (c_ref, c_buf), (w_ref, w_buf), (p_ref, p_buf))):
            view = src.at[pl.ds(at, SUB), :] if n == 3 else src.at[:, pl.ds(at, SUB), :]
            copies.append(pltpu.make_async_copy(view, dst.at[side], sems.at[side, n]))
    copies.append(pltpu.make_async_copy(mask_ref, mask_buf, more_sems.at[0]))
    copies.append(pltpu.make_async_copy(levels_ref, levels_buf, more_sems.at[1]))
    for copy in copies:
        copy.start()
    for copy in copies:
        copy.wait()
    set_film(mask_buf, film_ref)

    def fill(out, side, near, far):
        for l in range(layers):
            out[l : l + 1, :] = s_buf[side, l, near : near + 1, :]
            out[layers + l : layers + l + 1, :] = s_buf[side, l, far : far + 1, :]
            out[2 * layers + l : 2 * layers + l + 1, :] = c_buf[side, l, near : near + 1, :]
        for k in range(chans):
            out[3 * layers + k : 3 * layers + k + 1, :] = w_buf[side, k, near : near + 1, :]
        heat = looked_up(p_buf[side, near : near + 1, :], levels_buf)
        for k in range(chans):
            out[3 * layers + chans + k : 3 * layers + chans + k + 1, :] = heat

    par = parity("flow")

    @pl.when(par == 0)
    def _():
        fill(even_ref, 1, 7, 6)
        fill(odd_ref, 0, 0, 1)

    @pl.when(par != 0)
    def _():
        fill(odd_ref, 1, 7, 6)
        fill(even_ref, 0, 0, 1)


def set_film(mask_ref, film):
    for k in range(mask_ref.shape[0]):
        row = mask_ref[k : k + 1, :].astype(jnp.float32) * FILM
        film[k] = jnp.broadcast_to(row, film.shape[1:])


def stencil(l, load, c_ref, w_ref, film, a_ref, make, top, bottom, emit, length, layers, tiles):
    row, lane = iota(0), iota(1)
    zero = jnp.zeros((SUB, LANES), jnp.float32)
    k = l // 2
    above_l, below_l = jnp.maximum(l - 1, 0), jnp.minimum(l + 1, layers - 1)
    f = [film[k, :, cut(c)] for c in range(tiles)]
    keep = [(1.0 - 2.0 * VERTICAL) - v for v in f]
    count = length // SUB
    down = lambda v: pltpu.roll(v, 1, 0)
    up = lambda v: pltpu.roll(v, SUB - 1, 0)
    if top is None:
        before = [jnp.zeros((SUB, LANES), jnp.float32)] * tiles
        final = before
    else:
        before = [top[l, :, cut(c)] for c in range(tiles)]
        final = None
    u = [load(l, 0, c) for c in range(tiles)]
    u_up = [up(v) for v in u]
    for r in range(count):
        if r + 1 < count:
            after = [load(l, (r + 1) * SUB, c) for c in range(tiles)]
            after_up = [up(v) for v in after]
        elif final is None:
            after = [bottom[l, :, cut(c)] for c in range(tiles)]
            after_up = after
        else:
            after = after_up = final
        u_down = [down(v) for v in u]
        east = [pltpu.roll(v, 1, 1) for v in u]
        west = [pltpu.roll(v, LANES - 1, 1) for v in u]
        at = r * SUB
        conds, outs, ws = [], [], []
        for c in range(tiles):
            n = jnp.where(row == 0, before[c], u_down[c])
            s = jnp.where(row == SUB - 1, after_up[c], u_up[c])
            lf = jnp.where(lane == 0, zero if c == 0 else east[c - 1], east[c])
            rt = jnp.where(lane == LANES - 1, zero if c == tiles - 1 else west[c + 1], west[c])
            cond = c_ref[l, at : at + SUB, cut(c)]
            w = w_ref[k, at : at + SUB, cut(c)]
            if make:
                own = keep[c] - 4.0 * cond
                a_ref[l, at : at + SUB, cut(c)] = own
            else:
                own = a_ref[l, at : at + SUB, cut(c)]
            beside = load(above_l, at, c) + load(below_l, at, c)
            outs.append((own * u[c] + cond * ((n + s) + (lf + rt))) + (VERTICAL * beside + f[c] * w))
            conds.append(cond)
            ws.append(w)
        emit(r, u, conds, outs, ws)
        before, u, u_up = u_down, after, after_up


def first_step(levels_ref, s_ref, c_ref, w_ref, p_ref, film, s1_ref, a_ref, heat_ref, flat_ref):
    layers, length, width = s_ref.shape
    tiles = width // LANES
    zero = jnp.zeros((SUB, LANES), jnp.float32)

    def layer(l, carry):
        def load(m, at, c):
            return s_ref[m, at : at + SUB, cut(c)]

        def emit(r, u, conds, outs, ws):
            at = r * SUB
            for c in range(tiles):
                s1_ref[l, at : at + SUB, cut(c)] = outs[c]

        stencil(l, load, c_ref, w_ref, film, a_ref, True, None, None, emit, length, layers, tiles)
        return carry

    lax.fori_loop(0, layers, layer, 0)
    table = zero
    for n in range(levels_ref.shape[0]):
        table = jnp.where(iota(1) == n, levels_ref[n], table)
    for r in range(length // SUB):
        at = r * SUB
        for c in range(tiles):
            heat = jnp.take_along_axis(table, p_ref[at : at + SUB, cut(c)], axis=1)
            heat_ref[at : at + SUB, cut(c)] = heat
            s1_ref[0, at : at + SUB, cut(c)] += heat
    lane = lax.broadcasted_iota(jnp.int32, (length, LANES), 1)
    for n, ref in enumerate((s_ref, c_ref, s1_ref)):
        for l in range(layers):
            turned = jnp.where(lane < LANES // 2, ref[l, :, cut(0)], ref[l, :, cut(tiles - 1)]).T
            j = n * SUB + l
            flat_ref[j : j + 1, :] = turned[0:1, :]
            flat_ref[j + 64 : j + 65, :] = turned[LANES - 1 :, :]
            if n == 1:
                flat_ref[j + 16 : j + 17, :] = turned[1:2, :]
                flat_ref[j + 80 : j + 81, :] = turned[LANES - 2 : LANES - 1, :]


def add_rows(s_ref, c_ref, film, re_ref, ro_ref, flat_ref, s1_in, s1_ref, halo_ref, even_ref, odd_ref, rows):
    layers, length, width = s_ref.shape
    chans = film.shape[0]
    tiles = width // LANES
    last = tiles - 1
    row, lane = iota(0), iota(1)
    zero = jnp.zeros((SUB, LANES), jnp.float32)
    fpar, cpar = parity("flow"), parity("cross")
    for l in range(layers):
        rows[0, l : l + 1, :] = s_ref[l, 0:1, :]
        rows[1, l : l + 1, :] = s_ref[l, length - 1 : length, :]
        rows[2, l : l + 1, :] = film[l // 2, 0:1, :]

    top = lambda a, b, c: jnp.where(fpar == 0, ro_ref[a:b, cut(c)], re_ref[a:b, cut(c)])
    bottom = lambda a, b, c: jnp.where(fpar == 0, re_ref[a:b, cut(c)], ro_ref[a:b, cut(c)])
    nears = []
    for side, halo in ((0, top), (1, bottom)):
        near = [halo(0, layers, c) for c in range(tiles)]
        nears.append(near)
        east = [pltpu.roll(v, 1, 1) for v in near]
        west = [pltpu.roll(v, LANES - 1, 1) for v in near]
        at = 0 if side == 0 else length - SUB
        for c in range(tiles):
            cond = halo(2 * layers, 3 * layers, c)
            rest = halo(3 * layers, 4 * layers, c)
            heat = jnp.where(row == 0, jnp.broadcast_to(rest[chans : chans + 1, :], (SUB, LANES)), 0.0)
            cool = zero
            for k in range(chans):
                cool = jnp.where(row // 2 == k, jnp.broadcast_to(rest[k : k + 1, :], (SUB, LANES)), cool)
            u = near[c]
            lf = jnp.where(lane == 0, zero if c == 0 else east[c - 1], east[c])
            rt = jnp.where(lane == LANES - 1, zero if c == last else west[c + 1], west[c])
            around = (halo(layers, 2 * layers, c) + rows[side, :, cut(c)]) + (lf + rt)
            over = jnp.where(row == 0, u, pltpu.roll(u, 1, 0))
            under = jnp.where(row == SUB - 1, u, pltpu.roll(u, SUB - 1, 0))
            halo_ref[side * layers : (side + 1) * layers, cut(c)] = (
                u
                + cond * (around - 4.0 * u)
                + VERTICAL * ((over - u) + (under - u))
                + rows[2, :, cut(c)] * (cool - u)
                + heat
            )
            spot = 0 if side == 0 else SUB - 1
            for l in range(layers):
                outside = jnp.broadcast_to(u[l : l + 1, :], (SUB, LANES))
                more = jnp.where(row == spot, c_ref[l, at : at + SUB, cut(c)] * outside, 0.0)
                s1_ref[l, at : at + SUB, cut(c)] = s1_in[l, at : at + SUB, cut(c)] + more

    back = LANES - 1
    def fill(right_ref, left_ref):
        for is_left, out in ((0, right_ref), (1, left_ref)):
            base = 0 if is_left else 64
            tile = 0 if is_left else last
            out[0:16, :] = flat_ref[base : base + 16, :]
            t, b = nears[0][tile], nears[1][tile]
            t0 = t if is_left else pltpu.roll(t, 1, 1)
            b1 = pltpu.roll(b, back, 1) if is_left else b
            out[16:24, 0:LANES] = flat_ref[base + 16 : base + 24, 0:LANES] + jnp.where(
                lane == 0, flat_ref[base + 8 : base + 16, 0:LANES] * t0, 0.0
            )
            out[16:24, LANES:] = flat_ref[base + 16 : base + 24, LANES:] + jnp.where(
                lane == back, flat_ref[base + 8 : base + 16, LANES:] * b1, 0.0
            )
            shift = back if is_left else 1
            out[24:32, 0:LANES] = pltpu.roll(t, shift, 1)
            out[24:32, LANES:] = pltpu.roll(b, shift, 1)

    @pl.when(cpar == 0)
    def _():
        fill(even_ref, odd_ref)

    @pl.when(cpar != 0)
    def _():
        fill(odd_ref, even_ref)


def second_step(
    s1_ref, c_ref, w_ref, heat_ref, film, a_ref, halo_ref, s2_ref, kept_ref, base_ref, top, bottom, sums_ref, out_buf, sem
):
    layers, length, width = s1_ref.shape
    chans = w_ref.shape[0]
    tiles = width // LANES
    zero = jnp.zeros((SUB, LANES), jnp.float32)
    for at, out in ((0, top), (1, bottom)):
        for l in range(layers):
            out[l] = jnp.broadcast_to(halo_ref[at * layers + l : at * layers + l + 1, :], (SUB, width))
    sums_ref[...] = jnp.zeros(sums_ref.shape, jnp.float32)

    def layer(l, carry):
        sums = [zero] * tiles

        def load(m, at, c):
            return s1_ref[m, at : at + SUB, cut(c)]

        def emit(r, u, conds, outs, ws):
            at = r * SUB
            for c in range(tiles):
                out_buf[l, at : at + SUB, cut(c)] = outs[c]
                sums[c] = sums[c] + (outs[c] - ws[c])

        stencil(l, load, c_ref, w_ref, film, a_ref, False, top, bottom, emit, length, layers, tiles)
        for c in range(tiles):
            sums_ref[l // 2, :, cut(c)] += sums[c]

        @pl.when(l == 0)
        def _():
            for c in range(tiles):
                total = zero
                for r in range(length // SUB):
                    at = r * SUB
                    heat = heat_ref[at : at + SUB, cut(c)]
                    out_buf[0, at : at + SUB, cut(c)] += heat
                    total = total + heat
                sums_ref[0, :, cut(c)] += total

        @pl.when(l < layers - 2)
        def _():
            pltpu.make_async_copy(out_buf.at[l], s2_ref.at[l], sem.at[l]).start()

        return carry

    lax.fori_loop(0, layers, layer, 0)
    kept_ref[...] = out_buf[layers - 2 :]
    for k in range(chans):
        base_ref[k : k + 1, :] = jnp.sum(sums_ref[k] * film[k], axis=0, keepdims=True)
    for l in range(layers - 2):
        pltpu.make_async_copy(out_buf.at[l], s2_ref.at[l], sem.at[l]).wait()


def add_columns(film, re_ref, ro_ref, ce_ref, co_ref, own_ref, base_ref, total_ref, change_ref):
    layers = SUB
    chans = film.shape[0]
    tiles = base_ref.shape[1] // LANES
    halves = change_ref.shape[1] // LANES
    row, lane = iota(0), iota(1)
    end = LANES - 1
    fpar, cpar = parity("flow"), parity("cross")

    def rolled(v, by):
        return pltpu.roll(v, by, 1)

    sums = []
    for side in range(2):
        spot, tile, base = (0, 0, 0) if side == 0 else (end, tiles - 1, 64)

        def got(a, h, side=side):
            ours, theirs = (co_ref, ce_ref) if side == 0 else (ce_ref, co_ref)
            return jnp.where(cpar == 0, ours[a : a + SUB, cut(h)], theirs[a : a + SUB, cut(h)])

        cond_top = jnp.where(fpar == 0, ro_ref[16:24, cut(tile)], re_ref[16:24, cut(tile)])
        cond_bottom = jnp.where(fpar == 0, re_ref[16:24, cut(tile)], ro_ref[16:24, cut(tile)])
        cond = [own_ref[base + 8 : base + 16, cut(h)] for h in range(halves)]
        first = [cond[h] * got(0, h) for h in range(halves)]
        before, after = cond_top * got(24, 0), cond_bottom * got(24, 1)
        if side == 0:
            after = rolled(after, end)
        else:
            before = rolled(before, 1)
        f = jnp.zeros((SUB, LANES), jnp.float32)
        for k in range(chans):
            f = jnp.where(row // 2 == k, film[k, :, cut(tile)], f)
        keep = (1.0 - 2.0 * VERTICAL) - jnp.broadcast_to(f[:, spot : spot + 1], (SUB, LANES))
        outer_sum = inner_sum = jnp.zeros((SUB, LANES), jnp.float32)
        for h in range(halves):
            d = first[h]
            n = jnp.where(lane == 0, before if h == 0 else rolled(first[h - 1], 1), rolled(d, 1))
            s = jnp.where(lane == end, after if h == halves - 1 else rolled(first[h + 1], end), rolled(d, end))
            beyond = got(16, h) + got(8, h) * own_ref[base : base + 8, cut(h)]
            over = jnp.where(row == 0, d, pltpu.roll(d, 1, 0))
            under = jnp.where(row == SUB - 1, d, pltpu.roll(d, SUB - 1, 0))
            outer = keep * d + cond[h] * (((n + s) + beyond) - 4.0 * d) + VERTICAL * (over + under)
            inner = own_ref[base + 24 : base + 32, cut(h)] * d
            at = 2 * layers * side
            change_ref[at : at + layers, cut(h)] = outer if side == 0 else inner
            change_ref[at + layers : at + 2 * layers, cut(h)] = inner if side == 0 else outer
            outer_sum, inner_sum = outer_sum + outer, inner_sum + inner
        outer_sum = jnp.broadcast_to(jnp.sum(outer_sum, axis=1, keepdims=True), (SUB, LANES))
        inner_sum = jnp.broadcast_to(jnp.sum(inner_sum, axis=1, keepdims=True), (SUB, LANES))
        inner_spot = 1 if side == 0 else end - 1
        both = jnp.where(lane == spot, outer_sum, jnp.where(lane == inner_spot, inner_sum, 0.0))
        sums.append(both + pltpu.roll(both, SUB - 1, 0))
    for k in range(chans):
        for c in range(tiles):
            value = base_ref[k : k + 1, cut(c)]
            if c in (0, tiles - 1):
                value = value + film[k, 0:1, cut(c)] * sums[0 if c == 0 else 1][2 * k : 2 * k + 1, :]
            for j in range(total_ref.shape[0]):
                total_ref[j, 0, k : k + 1, cut(c)] = value


def march(
    length_cells, s_in, w_ref, kept_ref, change_ref, mask_ref, inlet_ref, gain_ref, s2_ref, part_ref, s_buf, w_buf, in_sem, out_sem
):
    chans, length, width = part_ref.shape
    tiles = width // LANES
    row, lane = iota(0), lax.broadcasted_iota(jnp.int32, (length, LANES), 1)
    reads, writes = [], []
    for k in range(chans):
        pair = pl.ds(2 * k, 2)
        reads.append(pltpu.make_async_copy(w_ref.at[k], w_buf.at[k], in_sem.at[1, k]))
        if k < chans - 1:
            reads.append(pltpu.make_async_copy(s_in.at[pair], s_buf.at[pair], in_sem.at[0, k]))
    for copy in reads:
        copy.start()
    s_buf[2 * chans - 2 :] = kept_ref[...]
    i = lax.broadcasted_iota(jnp.int32, (length, length), 0)
    j = lax.broadcasted_iota(jnp.int32, (length, length), 1)
    triangle = jnp.where(j < i, 1.0, jnp.where(j == i, 0.5, 0.0)).astype(jnp.bfloat16)
    middle = jnp.zeros((LANES - 2 * SUB, length), jnp.float32)
    rows = lax.broadcasted_iota(jnp.int32, (SUB, length), 0)
    for k in range(chans):
        for copy in reads[2 * k : 2 * k + 2]:
            copy.wait()
        for l in (2 * k, 2 * k + 1):
            line = lambda n: jnp.broadcast_to(change_ref[n * SUB + l : n * SUB + l + 1, :], (SUB, length))
            first = jnp.where(rows == 0, line(0), jnp.where(rows == 1, line(1), 0.0))
            final = jnp.where(rows == SUB - 2, line(2), jnp.where(rows == SUB - 1, line(3), 0.0))
            turned = jnp.concatenate([first, middle, final], axis=0).T
            s_buf[l, :, cut(0)] += jnp.where(lane < 2, turned, 0.0)
            s_buf[l, :, cut(tiles - 1)] += jnp.where(lane >= LANES - 2, turned, 0.0)
            for side in range(2 if k < chans - 1 else 1):
                view = (l, slice(None), cut(side * (tiles - 1)) if k < chans - 1 else slice(None))
                writes.append(pltpu.make_async_copy(s_buf.at[view], s2_ref.at[view], out_sem.at[side, l]))
                writes[-1].start()
        f = mask_ref[k : k + 1, :].astype(jnp.float32) * FILM
        absorbed = f * ((s_buf[2 * k] + s_buf[2 * k + 1]) - 2.0 * w_buf[k])
        within = None
        for _ in range(3):
            term = absorbed.astype(jnp.bfloat16)
            absorbed = absorbed - term.astype(jnp.float32)
            product = jnp.dot(triangle, term, preferred_element_type=jnp.float32)
            within = product if within is None else within + product
        scale = gain_ref[k : k + 1, :] * (1.0 / length_cells)
        part_ref[k] = inlet_ref[k : k + 1, :] + scale * within
    for copy in writes:
        copy.wait()


def finish(length_cells, part_ref, every_ref, gain_ref, out_ref, buf, sem):
    flow = lax.axis_index("flow")
    total = jnp.zeros(gain_ref.shape, jnp.float32)
    for j in range(every_ref.shape[0]):
        total += jnp.where(j < flow, every_ref[j, 0], 0.0)
    carried = total * gain_ref[...] * (1.0 / length_cells)
    chans = part_ref.shape[0]
    copies = []
    for k in range(chans):
        buf[k] = part_ref[k] + carried[k : k + 1, :]
        copies.append(pltpu.make_async_copy(buf.at[k], out_ref.at[k], sem.at[k]))
        copies[-1].start()
    for copy in copies:
        copy.wait()


def swaps(size):
    even = [(i, i ^ 1) for i in range(size)]
    odd = [(i, i + 1 if i % 2 else i - 1) for i in range(1, size - 1)]
    return even, odd


def f32(*dims):
    return jax.ShapeDtypeStruct(dims, jnp.float32)


def call(kernel, name, out_shape, in_specs, out_specs, scratch, mib, flops, **kw):
    return pl.pallas_call(
        kernel,
        out_shape=out_shape,
        in_specs=in_specs,
        out_specs=out_specs,
        scratch_shapes=scratch,
        compiler_params=pltpu.CompilerParams(vmem_limit_bytes=int(mib * 2**20)),
        cost_estimate=pl.CostEstimate(flops=int(flops), bytes_accessed=0, transcendentals=0),
        name=name,
        **kw,
    )


def shards(s0, cond, cool, index, levels, mask, inlet, gain):
    layers, length, width = s0.shape
    chans = cool.shape[0]
    flows = lax.axis_size("flow")
    count = 4 * layers
    block = f32(layers, length, width)
    buf = lambda *dims: pltpu.VMEM(dims, jnp.float32)
    hbm = lambda *dims: pltpu.HBM(dims, jnp.float32)
    dma = lambda *dims: pltpu.SemaphoreType.DMA(dims)
    in_hbm = lambda x: pltpu.with_memory_space_constraint(x, pltpu.HBM)
    even, odd, film = call(
        edge_rows, "edge_rows", (f32(count, width), f32(count, width), f32(chans, SUB, width)), [HBM] * 6, (VMEM,) * 3,
        [
            buf(2, layers, SUB, width), buf(2, layers, SUB, width), buf(2, chans, SUB, width),
            pltpu.VMEM((2, SUB, width), jnp.int32), pltpu.VMEM(mask.shape, jnp.int32),
            pltpu.SMEM(levels.shape, jnp.float32), dma(2, 4), dma(2),
        ],
        4, 1e5,
    )(*map(in_hbm, (levels, s0, cond, cool, index, mask)))
    even_pairs, odd_pairs = swaps(flows)
    row_odd = lax.ppermute(odd, "flow", odd_pairs)
    row_even = lax.ppermute(even, "flow", even_pairs)

    work = 20 * layers * length * width
    s1, factor, heat, own = call(
        first_step, "first_step", (block, block, f32(length, width), f32(LANES, length)), [SMEM] + [VMEM] * 5, (VMEM,) * 4,
        [], 21, work,
    )(levels, s0, cond, cool, index, film)
    s1, halo, even, odd = call(
        add_rows, "add_rows", (block, f32(2 * layers, width), f32(32, length), f32(32, length)), [VMEM] * 7, (VMEM,) * 4,
        [buf(3, layers, width)], 17, 1e5, input_output_aliases={6: 0},
    )(s0, cond, film, row_even, row_odd, own, s1)
    even_pairs, odd_pairs = swaps(lax.axis_size("cross"))
    col_odd = lax.ppermute(odd, "cross", odd_pairs)
    col_even = lax.ppermute(even, "cross", even_pairs)

    s2, kept, base = call(
        second_step, "second_step", (hbm(layers, length, width), f32(2, length, width), f32(chans, width)), [VMEM] * 7,
        (HBM, VMEM, VMEM),
        [
            buf(layers, SUB, width), buf(layers, SUB, width), buf(chans, SUB, width), buf(layers, length, width),
            dma(layers),
        ],
        23, work,
    )(s1, cond, cool, heat, film, factor, halo)
    totals, change = call(
        add_columns, "add_columns", (f32(flows, 1, chans, width), f32(32, length)), [VMEM] * 7, (VMEM, VMEM), [], 4, 1e4,
    )(film, row_even, row_odd, col_even, col_odd, own, base)
    everyone = lax.all_to_all(totals, "flow", 0, 0, tiled=True)

    cells = float(length * flows)
    s2, part = call(
        functools.partial(march, cells), "march", (hbm(layers, length, width), f32(chans, length, width)),
        [HBM, HBM] + [VMEM] * 5, (HBM, VMEM),
        [buf(layers, length, width), buf(chans, length, width), dma(2, chans), dma(2, layers)],
        14, work // 4, input_output_aliases={0: 0},
    )(in_hbm(s2), in_hbm(cool), kept, change, mask, inlet, gain)
    fluid = call(
        functools.partial(finish, cells), "finish", hbm(chans, length, width), [VMEM] * 3, HBM,
        [buf(chans, length, width), dma(chans)], 6, 1e5,
    )(part, everyone, gain)
    return s2, fluid


def solution(mesh):
    return jax.shard_map(
        shards,
        mesh=mesh,
        in_specs=(
            P(None, "flow", "cross"),
            P(None, "flow", "cross"),
            P(None, "flow", "cross"),
            P("flow", "cross"),
            P(),
            P(None, "cross"),
            P(None, "cross"),
            P(None, "cross"),
        ),
        out_specs=(P(None, "flow", "cross"), P(None, "flow", "cross")),
        check_vma=False,
    )
```
